32 devices in a mesh: shard: 8 (over z, x), width: 4 (over y, core).
Axes of the slice: x: 2, y: 2, z: 4, core: 2. Of those that a mesh axis runs over, the one named last changes fastest.
Arguments:
- w_gate: bfloat16 [2048, 8192], P('shard', 'width'), may hold values from -0.125 to 0.125
- low_gate: bfloat16 [2048, 64], P('shard'), may hold values from -0.125 to 0.125
- high_gate: bfloat16 [64, 8192], P(None, 'width'), may hold values from -0.75 to 0.75
- w_up: bfloat16 [2048, 8192], P('shard', 'width'), may hold values from -0.125 to 0.125
- low_up: bfloat16 [2048, 64], P('shard'), may hold values from -0.125 to 0.125
- high_up: bfloat16 [64, 8192], P(None, 'width'), may hold values from -0.75 to 0.75
- w_down: bfloat16 [8192, 2048], P('width', 'shard'), may hold values from -0.0625 to 0.0625
- low_down: bfloat16 [8192, 64], P('width'), may hold values from -0.0625 to 0.0625
- high_down: bfloat16 [64, 2048], P(None, 'shard'), may hold values from -0.75 to 0.75
- norm_train: float32 [2048], P(('shard', 'width')), may hold values from 0.25 to 1.75
- norm_step: float32 [2048], P(('shard', 'width')), may hold values from -0.3 to 0.3
Outputs:
- serve_gate: bfloat16 [8192, 2048], P('width')
- serve_up: bfloat16 [8192, 2048], P('width')
- serve_down: bfloat16 [2048, 8192], P(None, 'width')
- serve_norm: bfloat16 [2048], replicated
The draws below stay inside these ranges and needn't reach their ends.
All inputs are finite; a program needn't handle non-finite values.
Results may differ from the reference program's by a relative error of at most 0.001.
Values may be sent and summed in bfloat16 or wider, within the bound.
No kernel may reach another device: no remote copies, remote signals or barrier semaphores. Data moves between devices by JAX's collectives and lax.ppermute only.
A program may use at most 128 MiB of HBM per device.

```python
import jax
import jax.numpy as jnp

D_MODEL = 2048
D_INNER = 8192
RANK = 64


def level_of(own_key, extent, cuts, smallest, largest):
    factor_of, own = 1.0, jax.random.fold_in(own_key, 6)
    for dim, shards_of in cuts:
        steps = jnp.exp(jax.random.uniform(jax.random.fold_in(own, dim), (shards_of,), jnp.float32, smallest / len(cuts), largest / len(cuts)))
        factor_of = factor_of * jnp.repeat(steps, extent[dim] // shards_of).reshape([-1 if axis == dim else 1 for axis in range(len(extent))])
    return factor_of


def gaussian(stream_key, extent, deviation, reach, pieces=(), dtype=jnp.bfloat16):
    drawn = deviation * jax.random.normal(stream_key, extent, jnp.float32)
    if pieces:
        drawn = drawn * level_of(stream_key, extent, pieces, -0.22, 0.18)
    return jnp.clip(drawn, -reach, reach).astype(dtype)


def setup_inputs(seed: int = 0) -> dict:
    key_list = jax.random.split(jax.random.key(seed), 12)
    w_gate = gaussian(key_list[0], (D_MODEL, D_INNER), D_MODEL ** -0.5, 0.125, ((0, 8), (1, 4)))
    low_gate = gaussian(key_list[1], (D_MODEL, RANK), D_MODEL ** -0.5, 0.125, ((0, 8),))
    high_gate = gaussian(key_list[2], (RANK, D_INNER), RANK ** -0.5, 0.75, ((1, 4),))
    w_up = gaussian(key_list[3], (D_MODEL, D_INNER), D_MODEL ** -0.5, 0.125, ((0, 8), (1, 4)))
    low_up = gaussian(key_list[4], (D_MODEL, RANK), D_MODEL ** -0.5, 0.125, ((0, 8),))
    high_up = gaussian(key_list[5], (RANK, D_INNER), RANK ** -0.5, 0.75, ((1, 4),))
    w_down = gaussian(key_list[6], (D_INNER, D_MODEL), D_INNER ** -0.5, 0.0625, ((0, 4), (1, 8)))
    low_down = gaussian(key_list[7], (D_INNER, RANK), D_INNER ** -0.5, 0.0625, ((0, 4),))
    high_down = gaussian(key_list[8], (RANK, D_MODEL), RANK ** -0.5, 0.75, ((1, 8),))
    norm_train = jnp.clip(1.0 + 0.15 * jax.random.normal(key_list[9], (D_MODEL,), jnp.float32), 0.25, 1.75)
    norm_step = jnp.clip(jax.random.uniform(key_list[10], (D_MODEL,), jnp.float32, -0.3, 0.3) * level_of(key_list[10], (D_MODEL,), ((0, 32),), -0.4, 0.0), -0.3, 0.3)
    return {"w_gate": w_gate, "low_gate": low_gate, "high_gate": high_gate, "w_up": w_up, "low_up": low_up, "high_up": high_up, "w_down": w_down, "low_down": low_down, "high_down": high_down, "norm_train": norm_train, "norm_step": norm_step}


mix_rate = 2.0


def reference(w_gate, low_gate, high_gate, w_up, low_up, high_up, w_down, low_down, high_down, norm_train, norm_step):
    fresh_gate = w_gate.astype(jnp.float32) + mix_rate * jnp.dot(low_gate, high_gate, preferred_element_type=jnp.float32)
    fresh_up = w_up.astype(jnp.float32) + mix_rate * jnp.dot(low_up, high_up, preferred_element_type=jnp.float32)
    fresh_down = w_down.astype(jnp.float32) + mix_rate * jnp.dot(low_down, high_down, preferred_element_type=jnp.float32)
    serve_gate = fresh_gate.T.astype(jnp.bfloat16)
    serve_up = fresh_up.T.astype(jnp.bfloat16)
    serve_down = fresh_down.T.astype(jnp.bfloat16)
    serve_norm = (norm_train + norm_step).astype(jnp.bfloat16)
    return serve_gate, serve_up, serve_down, serve_norm
```

```python
import functools

import jax
import jax.numpy as jnp
from jax import lax
from jax.experimental import pallas as pl
from jax.experimental.pallas import tpu as pltpu
from jax.sharding import PartitionSpec as P

mix_rate = 2.0


def merged(w, low, high):
    return w.astype(jnp.float32) + mix_rate * jnp.dot(low, high, preferred_element_type=jnp.float32)


def merge_wide_kernel(full, wg, lg, hg, wu, lu, hu, out):
    j = pl.program_id(0)

    @pl.when(j < full)
    def _():
        out[...] = merged(wg[...], lg[...], hg[...]).T.astype(out.dtype)

    @pl.when(j >= full)
    def _():
        out[...] = merged(wu[...], lu[...], hu[...]).T.astype(out.dtype)


def merge_tall_kernel(part, wu, lu, hu, wd, ld, hd, out):
    j = pl.program_id(0)
    depth = out.shape[1]

    @pl.when(j < part)
    def _():
        out[...] = merged(wu[...], lu[...], hu[...]).T.astype(out.dtype)

    @pl.when(j >= part)
    def _():
        for b in range(out.shape[0] // depth):
            rows = pl.ds(b * depth, depth)
            out[rows, :] = merged(wd[rows, :], ld[rows, :], hd[...]).T.astype(out.dtype)


def merge_halves(wg, lg, hg, wu, lu, hu, wd, ld, hd):
    depth, inner = wg.shape
    rank = lg.shape[1]
    block = inner // 4
    whole = pl.BlockSpec((depth, rank), lambda j: (0, 0))
    rows = inner + inner // 2
    out = dict(
        out_shape=jax.ShapeDtypeStruct((rows, depth), wg.dtype),
        out_specs=pl.BlockSpec((block, depth), lambda j: (j, 0)),
        grid=(rows // block,),
    )
    params = pltpu.CompilerParams(vmem_limit_bytes=16 * 2**20)
    gate = lambda j: (0, jnp.minimum(j, 3))
    up = lambda j: (0, jnp.maximum(j - 4, 0))
    wide = pl.pallas_call(
        functools.partial(merge_wide_kernel, 4),
        in_specs=[
            pl.BlockSpec((depth, block), gate),
            whole,
            pl.BlockSpec((rank, block), gate),
            pl.BlockSpec((depth, block), up),
            whole,
            pl.BlockSpec((rank, block), up),
        ],
        compiler_params=params,
        name="merge_wide",
        **out,
    )(wg, lg, hg, wu, lu, hu)
    rest = lambda j: (0, jnp.minimum(j + 2, 3))
    down = lambda j: (jnp.maximum(j - 2, 0), 0)
    tall = pl.pallas_call(
        functools.partial(merge_tall_kernel, 2),
        in_specs=[
            pl.BlockSpec((depth, block), rest),
            whole,
            pl.BlockSpec((rank, block), rest),
            pl.BlockSpec((block, depth), down),
            pl.BlockSpec((block, rank), down),
            pl.BlockSpec((rank, depth), lambda j: (0, 0)),
        ],
        compiler_params=params,
        name="merge_tall",
        **out,
    )(wu, lu, hu, wd, ld, hd)
    return wide, tall


def place_kernel(items, n_bufs, *refs):
    bufs = refs[:n_bufs]
    gate, up, down = refs[-6:-3]
    held, in_sem, out_sem = refs[-3:]
    depth = held.shape[2]
    inner = gate.shape[0]
    me = lax.axis_index("shard")
    for k, (half, choices, source) in enumerate(items):
        for b, cond in choices:
            copy = pltpu.make_async_copy(bufs[b], held.at[k], in_sem.at[k])
            if cond is None:
                copy.start()
            else:
                pl.when(cond(me))(copy.start)
    stores = []
    for k, (half, choices, source) in enumerate(items):
        pltpu.make_async_copy(bufs[choices[0][0]], held.at[k], in_sem.at[k]).wait()
        at = pl.multiple_of(source(me) * depth, depth)
        cols = pl.ds(at, depth)
        if half == 0:
            parts = [
                (held.at[k, pl.ds(0, inner)], gate.at[:, cols]),
                (held.at[k, pl.ds(inner, inner // 2)], up.at[pl.ds(0, inner // 2), cols]),
            ]
        else:
            parts = [(held.at[k, pl.ds(0, inner // 2)], up.at[pl.ds(inner // 2, inner // 2), cols])]
            for b in range(inner // depth):
                parts.append(
                    (
                        held.at[k, pl.ds(inner // 2 + b * depth, depth)],
                        down.at[cols, pl.ds(b * depth, depth)],
                    )
                )
        for p, (src, dst) in enumerate(parts):
            copy = pltpu.make_async_copy(src, dst, out_sem.at[k, p])
            copy.start()
            stores.append(copy)
    for copy in stores:
        copy.wait()


def place(outs, items, shapes):
    bufs = []
    for _, choices, _ in items:
        for b, _ in choices:
            bufs.append(b)
    listed, k = [], 0
    for half, choices, source in items:
        here = []
        for _, cond in choices:
            here.append((k, cond))
            k += 1
        listed.append((half, here, source))
    hbm = pl.BlockSpec(memory_space=pltpu.HBM)
    rows, depth = bufs[0].shape
    n = len(bufs)
    given = list(outs) if outs is not None else []
    return pl.pallas_call(
        functools.partial(place_kernel, listed, n),
        out_shape=shapes,
        in_specs=[hbm] * (n + len(given)),
        out_specs=[hbm] * 3,
        scratch_shapes=[
            pltpu.VMEM((len(items), rows, depth), bufs[0].dtype),
            pltpu.SemaphoreType.DMA((len(items),)),
            pltpu.SemaphoreType.DMA((len(items), 9)),
        ],
        input_output_aliases={n + i: i for i in range(len(given))},
        compiler_params=pltpu.CompilerParams(vmem_limit_bytes=12 * 2**20),
        cost_estimate=pl.CostEstimate(flops=0, bytes_accessed=4 * rows * depth * len(items), transcendentals=0),
        name="place",
    )(*bufs, *given)


def gather_norm(value, sizes):
    total = sizes[0] * sizes[1]
    me = lax.axis_index("shard") * sizes[1] + lax.axis_index("width")
    step = 1
    while step < total:
        other = lax.ppermute(value, ("shard", "width"), [(i, i ^ step) for i in range(total)])
        first = (me // step) % 2 == 0
        value = jnp.where(first, jnp.concatenate([value, other]), jnp.concatenate([other, value]))
        step *= 2
    return value


def line_body(sizes, *args):
    norm_train, norm_step = args[9:]
    low, high = merge_halves(*args[:9])
    depth, inner = args[0].shape
    shapes = [
        jax.ShapeDtypeStruct((inner, depth * sizes[0]), args[0].dtype),
        jax.ShapeDtypeStruct((inner, depth * sizes[0]), args[0].dtype),
        jax.ShapeDtypeStruct((depth * sizes[0], inner), args[0].dtype),
    ]
    at = lambda z, x: 2 * z + x
    z_of, x_of = (lambda s: s // 2), (lambda s: s % 2)

    def along(moves):
        return [(at(a, x), at(b, x)) for a, b in moves for x in range(2)]

    def across(rows):
        return [(at(z, x), at(z, 1 - x)) for z in rows for x in range(2)]

    def send(value, pairs, name):
        with jax.named_scope(name):
            return lax.ppermute(value, "shard", pairs)

    outer_swap = along([(0, 1), (1, 0), (2, 3), (3, 2)])
    middle_swap = along([(1, 2), (2, 1)])
    outward = along([(1, 0), (2, 3)])
    inward = along([(0, 1), (3, 2)])
    every, ends, middles = across(range(4)), across((0, 3)), across((1, 2))

    is_end = lambda s: jnp.logical_or(s // 2 == 0, s // 2 == 3)
    is_mid = lambda s: jnp.logical_not(is_end(s))
    flip = lambda s: s + 1 - 2 * (s % 2)
    same = lambda s: s
    near = lambda s: at(z_of(s) + 1 - 2 * (z_of(s) % 2), x_of(s))
    second = lambda s: jnp.where(is_end(s), at((z_of(s) + 2) % 4, x_of(s)), at(3 - z_of(s), x_of(s)))
    third = lambda s: jnp.where(is_end(s), at(3 - z_of(s), x_of(s)), at((z_of(s) + 2) % 4, x_of(s)))
    other = lambda f: (lambda s: flip(f(s)))

    a1, b1, x0 = [None] * 2, [None] * 2, [None] * 2
    for h, value in enumerate((low, high)):
        a1[h] = send(value, outer_swap, f"a1_{h}")
        x0[h] = send(value, every, f"x0_{h}")
        b1[h] = send(value, middle_swap, f"b1_{h}")
    norm = gather_norm((norm_train + norm_step).astype(low.dtype), sizes)
    a2l = send(b1[0], outward, "a2_0")
    xa1l = send(a1[0], every, "xa1_0")
    b2l = send(a1[0], middle_swap, "b2_0")
    outs = place(None, [(0, [(low, None)], same), (1, [(high, None)], same), (0, [(a1[0], None)], near), (0, [(x0[0], None)], flip)], shapes)
    a2h = send(b1[1], outward, "a2_1")
    xa1h = send(a1[1], ends, "xa1_1")
    xb1l = send(b1[0], middles, "xb1_0")
    c1 = send(x0[1], inward, "c1")
    b2h = send(a1[1], middle_swap, "b2_1")
    outs = place(outs, [(1, [(a1[1], None)], near), (1, [(x0[1], None)], flip)], shapes)
    a3l = send(b2l, outward, "a3_0")
    xa2l = send(a2l, ends, "xa2_0")
    xb1h = send(b1[1], middles, "xb1_1")
    c2 = send(c1, middle_swap, "c2")
    outs = place(
        outs,
        [(0, [(a2l, is_end), (b1[0], is_mid)], second), (0, [(xa1l, None)], other(near))],
        shapes,
    )
    a3h = send(b2h, outward, "a3_1")
    xa2h = send(a2h, ends, "xa2_1")
    xb2l = send(b2l, middles, "xb2_0")
    outs = place(
        outs,
        [(1, [(a2h, is_end), (b1[1], is_mid)], second), (1, [(xa1h, is_end), (c1, is_mid)], other(near))],
        shapes,
    )
    c3 = send(c2, outward, "c3")
    xa3l = send(a3l, ends, "xa3_0")
    outs = place(
        outs,
        [(0, [(a3l, is_end), (b2l, is_mid)], third), (0, [(xa2l, is_end), (xb1l, is_mid)], other(second))],
        shapes,
    )
    outs = place(
        outs,
        [(1, [(a3h, is_end), (b2h, is_mid)], third), (1, [(xa2h, is_end), (xb1h, is_mid)], other(second))],
        shapes,
    )
    outs = place(
        outs,
        [(0, [(xa3l, is_end), (xb2l, is_mid)], other(third)), (1, [(c3, is_end), (c2, is_mid)], other(third))],
        shapes,
    )
    return (*outs, norm)


def gather_body(*args):
    pieces = [merged(*args[3 * i : 3 * i + 3]).T.astype(args[0].dtype) for i in range(3)]
    gate, up = (lax.all_gather(p, "shard", axis=1, tiled=True) for p in pieces[:2])
    down = lax.all_gather(pieces[2], "shard", axis=0, tiled=True)
    norm = lax.all_gather((args[9] + args[10]).astype(gate.dtype), ("shard", "width"), axis=0, tiled=True)
    return gate, up, down, norm


def solution(mesh):
    sizes = (mesh.shape["shard"], mesh.shape["width"])
    body = functools.partial(line_body, sizes) if sizes == (8, 4) else gather_body
    return jax.shard_map(
        body,
        mesh=mesh,
        in_specs=(
            P("shard", "width"),
            P("shard", None),
            P(None, "width"),
            P("shard", "width"),
            P("shard", None),
            P(None, "width"),
            P("width", "shard"),
            P("width", None),
            P(None, "shard"),
            P(("shard", "width")),
            P(("shard", "width")),
        ),
        out_specs=(P("width", None), P("width", None), P(None, "width"), P()),
        check_vma=False,
    )
```
